32 devices in a mesh: blk: 8 (over y, x, core), col: 4 (over z).
Axes of the slice: x: 2, y: 2, z: 4, core: 2. Of those that a mesh axis runs over, the one named last changes fastest.
Arguments:
- samples: bfloat16 [2048, 768], P('blk'), may hold values from -3 to 3
- targets: float32 [2048, 256], P('blk'), may hold values from -6 to 6
- batch_index: int32 [1024], P('blk'), may hold values from 0 to 255
- centers: bfloat16 [4096, 768], P(('blk', 'col')), may hold values from -3 to 3
- weights: float32 [4096, 256], P(('blk', 'col')), may hold values from -6 to 6
- nystrom_index: int32 [1536], replicated, may hold values from 0 to 4095, as said below
- eigvecs: float32 [1536, 128], replicated, may hold values from -0.15625 to 0.15625
- coefficient: float32 [128], replicated, may hold values from 0.4 to 0.95
Outputs:
- residual: float32 [1024, 256], P(('blk', 'col'))
- new_weights: float32 [4096, 256], P(('blk', 'col'))
The draws below stay inside these ranges and needn't reach their ends.
Inputs may be any that keep to these rules, and one draw needn't show every extreme that they name: Batch row i is sample row (i // 128) * 256 + batch_index[i]. `nystrom_index`: 1536 distinct center rows.
All inputs are finite; a program needn't handle non-finite values.
Results may differ from the reference program's by a relative error of at most 0.0003.
The reference program's roundings to bfloat16 on the way (of `points`, `kernel`, `weights_low` and `resid_low`) count: a program that leaves them out, or rounds other values in their place, can miss the bound.
Values may be sent and summed in bfloat16 or wider, within the bound.
No kernel may reach another device: no remote copies, remote signals or barrier semaphores. Data moves between devices by JAX's collectives and lax.ppermute only.
A program may use at most 64 MiB of HBM per device.

```python
import math
import jax
import jax.numpy as jnp
from jax import lax

D = 768
C = 256
CEN_DEV = 128
BLK_ROWS = 128
SAMP_DEV = 256
NYS = 1536
TOPQ = 128
BATCH = 1024
SAMPLES = 2048
CENTERS = 4096
N_BLK = 8
N_COL = 4


latent_rank = 16


def point_rows(key, count, salt_value):
    basis = jax.random.normal(jax.random.fold_in(key, 9001), (D, latent_rank), jnp.float32)
    key_latent = jax.random.fold_in(key, salt_value)
    key_noise = jax.random.fold_in(key, salt_value + 1)
    latent = jax.random.normal(key_latent, (count, latent_rank), jnp.float32)
    noise_part = 2.0 * jax.random.normal(key_noise, (count, D), jnp.float32)
    values = (jnp.dot(latent, basis.T, precision=lax.Precision.HIGHEST) + noise_part) / math.sqrt(D)
    return jnp.clip(values, -3.0, 3.0)


def draw_samples(key, part):
    return point_rows(key, SAMPLES, 11).astype(jnp.bfloat16)


def draw_centers(key, part):
    return point_rows(key, CENTERS, 23).astype(jnp.bfloat16)


def draw_nystrom_index(key, part):
    order = jax.random.permutation(jax.random.fold_in(key, 37), CENTERS)
    return order[:NYS].astype(jnp.int32)


def set_ends(drawn, key, least, largest):
    spot = [jax.random.randint(jax.random.fold_in(key, axis), (), 0, length) for axis, length in enumerate(drawn.shape)]
    widest = drawn.shape.index(max(drawn.shape))
    neighbour = spot[:widest] + [(spot[widest] + 1) % drawn.shape[widest]] + spot[widest + 1:]
    return drawn.at[tuple(spot)].set(least).at[tuple(neighbour)].set(largest)


def levels(stream_key, shape, shards, smallest, high):
    def one(dim, blocks):
        heights = jax.random.uniform(jax.random.fold_in(jax.random.fold_in(stream_key, 6), dim), (blocks,), jnp.float32, smallest / len(shards), high / len(shards))
        return jnp.repeat(jnp.exp(heights), shape[dim] // blocks).reshape((-1,) + (1,) * (len(shape) - dim - 1))

    loudness = one(*shards[0])
    for cut in shards[1:]:
        loudness = loudness * one(*cut)
    return loudness


def centred(stream_key, shape, scale, bound, cuts=(), kind=jnp.bfloat16):
    entries = jax.random.normal(stream_key, shape, jnp.float32) * scale
    if len(cuts) > 0:
        entries = levels(stream_key, shape, cuts, -0.22, 0.18) * entries
    return jnp.clip(entries, min=-bound, max=bound).astype(kind)


def setup_inputs(seed: int = 0) -> dict:
    seeds = jax.random.split(jax.random.key(seed), 9)
    samples = draw_samples(jax.random.fold_in(seeds[8], 71), 0)
    targets = centred(seeds[1], (SAMPLES, C), 1.0, 6.0, ((0, 8),), jnp.float32)
    batch_index = set_ends(jax.random.randint(seeds[2], (BATCH,), 0, SAMP_DEV), jax.random.fold_in(seeds[2], 1), 0, SAMP_DEV - 1).astype(jnp.int32)
    centers = draw_centers(jax.random.fold_in(seeds[8], 71), 0)
    weights = centred(seeds[4], (CENTERS, C), 1.0, 6.0, ((0, 32),), jnp.float32)
    nystrom_index = draw_nystrom_index(jax.random.fold_in(seeds[8], 71), 0)
    eigvecs = centred(seeds[6], (NYS, TOPQ), NYS ** -0.5, 0.15625, (), jnp.float32)
    coefficient = jnp.clip(jax.random.uniform(seeds[7], (TOPQ,), jnp.float32, 0.4, 0.95), 0.4, 0.95)
    return {"samples": samples, "targets": targets, "batch_index": batch_index, "centers": centers, "weights": weights, "nystrom_index": nystrom_index, "eigvecs": eigvecs, "coefficient": coefficient}


spread = 1.0
shift_sq = 1.0
step_size = 4.0

def kernel_rows(points, centers):
    point_sq = lax.optimization_barrier(jnp.sum(jnp.square(points.astype(jnp.float32)), axis=1, keepdims=True))
    center_sq = lax.optimization_barrier(jnp.sum(jnp.square(centers.astype(jnp.float32)), axis=1))
    cross = lax.dot_general(points, centers, (((1,), (1,)), ((), ())), preferred_element_type=jnp.float32)
    dist_sq = point_sq + center_sq[None, :] - 2.0 * cross
    return jnp.exp(-jnp.sqrt(dist_sq + shift_sq) / spread).astype(jnp.bfloat16)

def reference(samples, targets, batch_index, centers, weights, nystrom_index, eigvecs, coefficient):
    owner_block = jnp.arange(BATCH, dtype=jnp.int32) // BLK_ROWS
    sample_row = (owner_block * SAMP_DEV + batch_index).astype(jnp.int32)
    points = jnp.take(samples, sample_row, axis=0)
    wanted = jnp.take(targets, sample_row, axis=0)
    weights_low = weights.astype(jnp.bfloat16)
    per_block = CEN_DEV * N_COL
    center_blocks = centers.reshape(N_BLK, per_block, D)
    weight_blocks = weights_low.reshape(N_BLK, per_block, C)

    def add_block(running, blocks_pair):
        center_part, weight_part = blocks_pair
        kernel = kernel_rows(points, center_part)
        return (running + jnp.dot(kernel, weight_part, preferred_element_type=jnp.float32), None)
    initial = jnp.zeros((BATCH, C), jnp.float32)
    prediction, _ = lax.scan(add_block, initial, (center_blocks, weight_blocks))
    residual = prediction - wanted
    resid_low = residual.astype(jnp.bfloat16)

    def grad_block(center_part):
        kernel = kernel_rows(points, center_part)
        return lax.dot_general(kernel, resid_low, (((0,), (0,)), ((), ())), preferred_element_type=jnp.float32)
    gradient = lax.map(grad_block, center_blocks).reshape(CENTERS, C)
    highest = lax.Precision.HIGHEST
    picked = jnp.take(gradient, nystrom_index, axis=0)
    projected = lax.dot_general(eigvecs, picked, (((0,), (0,)), ((), ())), precision=highest)
    correction = jnp.dot(eigvecs, coefficient[:, None] * projected, precision=highest)
    adjusted = gradient.at[nystrom_index].add(-correction)
    return (residual, weights - step_size * adjusted)
```

```python
import jax
import jax.numpy as jnp
from jax import lax
from jax.sharding import PartitionSpec as P

spread = 1.0
shift_sq = 1.0
step_size = 4.0


def swapped(block, distance):
    route = [(i, i ^ distance) for i in range(lax.axis_size("blk"))]
    return lax.ppermute(block, "blk", route)


def kernel_block(points, centers):
    point_sq = jnp.sum(jnp.square(points.astype(jnp.float32)), axis=1, keepdims=True)
    center_sq = jnp.sum(jnp.square(centers.astype(jnp.float32)), axis=1)
    cross = lax.dot_general(
        points, centers, (((1,), (1,)), ((), ())), preferred_element_type=jnp.float32
    )
    dist_sq = point_sq + center_sq[None, :] - 2.0 * cross
    return jnp.exp(-jnp.sqrt(dist_sq + shift_sq) / spread).astype(jnp.bfloat16)


def split(value, terms):
    pieces = []
    for _ in range(terms):
        piece = lax.reduce_precision(value, 8, 7)
        pieces.append(piece.astype(jnp.bfloat16))
        value = value - piece
    return pieces


def local(samples, targets, batch_index, centers, weights, nystrom_index, eigvecs, coefficient):
    blocks = lax.axis_size("blk")
    columns = lax.axis_size("col")
    chips = blocks // 2
    my_block = lax.axis_index("blk")
    my_column = lax.axis_index("col")
    blk_rows = batch_index.shape[0]
    n_center, depth = centers.shape
    width = weights.shape[1]
    share_rows = blk_rows // columns
    top = eigvecs.shape[1]

    own = jnp.concatenate([centers, weights.astype(jnp.bfloat16)], axis=1)
    packs = [own] + [swapped(own, 2 * s) for s in range(1, chips)]
    points = jnp.take(samples, batch_index, axis=0)
    points = jnp.concatenate([points, swapped(points, 1)], axis=0)

    pieces = jnp.concatenate(split(eigvecs, 3), axis=1)
    rows = jnp.concatenate(
        [((my_block ^ (2 * s)) * columns + my_column) * n_center + jnp.arange(n_center) for s in range(chips)]
    )
    chosen = (rows[:, None] == nystrom_index[None, :]).astype(jnp.bfloat16)
    eig_rows = jnp.dot(chosen, pieces, preferred_element_type=jnp.float32)
    eig_low = eig_rows.astype(jnp.bfloat16)
    own_eig = (
        eig_rows[:n_center, :top] + eig_rows[:n_center, top : 2 * top] + eig_rows[:n_center, 2 * top :]
    )

    kernels = [kernel_block(points, pack[:, :depth]) for pack in packs]
    kernel = jnp.concatenate(kernels, axis=1)
    right = jnp.concatenate([jnp.concatenate([pack[:, depth:] for pack in packs], axis=0), eig_low], axis=1)
    part = jnp.dot(kernel, right, preferred_element_type=jnp.float32)
    part = jnp.concatenate(
        [
            part[:, :width],
            part[:, width : width + top]
            + part[:, width + top : width + 2 * top]
            + part[:, width + 2 * top :],
        ],
        axis=1,
    )
    part = part[:blk_rows] + swapped(part[blk_rows:], 1)
    kernel_own = [kernels[0]] + [swapped(kernels[s], 2 * s) for s in range(1, chips)]

    shares = lax.all_to_all(part.reshape(columns, share_rows, width + top), "col", 0, 0)
    summed = jnp.sum(shares, axis=0)
    own_index = lax.dynamic_slice_in_dim(batch_index, my_column * share_rows, share_rows, 0)
    residual = summed[:, :width] - jnp.take(targets, own_index, axis=0)
    sent = jnp.concatenate([residual.astype(jnp.bfloat16)] + split(summed[:, width:], 2), axis=1)
    block = lax.all_gather(sent, "col", axis=0, tiled=True)
    held = jnp.stack([block] + [swapped(block, 2 * s) for s in range(1, chips)])
    held = jnp.stack([held, swapped(held, 1)], axis=1).reshape(blocks * blk_rows, width + 2 * top)

    left = jnp.concatenate([jnp.concatenate(kernel_own, axis=0), held[:, width:]], axis=1)
    product = lax.dot_general(
        left, held[:, :width], (((0,), (0,)), ((), ())), preferred_element_type=jnp.float32
    )
    gradient = product[:n_center]
    projected = product[n_center : n_center + top] + product[n_center + top :]
    correction = jnp.dot(own_eig, coefficient[:, None] * projected, precision=lax.Precision.HIGHEST)
    return (residual, weights - step_size * (gradient - correction))


def solution(mesh):
    in_specs = (
        P("blk", None),
        P("blk", None),
        P("blk"),
        P(("blk", "col"), None),
        P(("blk", "col"), None),
        P(),
        P(),
        P(),
    )
    out_specs = (P(("blk", "col"), None), P(("blk", "col"), None))
    return jax.shard_map(local, mesh=mesh, in_specs=in_specs, out_specs=out_specs, check_vma=False)
```
